32 devices in a mesh: member: 1, span: 32 (over z, y, x, core).
Axes of the slice: x: 2, y: 2, z: 4, core: 2. Of those that a mesh axis runs over, the one named last changes fastest.
Arguments:
- field: float32 [1024, 23040], P(('member', 'span')), may hold values from -60 to 60
- day_table: int32 [1024], P('member'), may hold values from 0 to 364
- band_owner: int32 [32], P('member'), may hold values from 0 to 31, as said below
- sea_mask: int32 [23040], replicated, may hold values 0 or 1
Outputs:
- coeff_out: float32 [13, 23040], P(None, ('member', 'span'))
- variance_out: float32 [23040], P(('member', 'span'))
The draws below stay inside these ranges and needn't reach their ends.
Inputs may be any that keep to these rules, and one draw needn't show every extreme that they name: `band_owner`: a permutation of 0 to 31.
All inputs are finite; a program needn't handle non-finite values.
Results may differ from the reference program's by a relative error of at most 0.00013.
Values sent between devices are 32-bit elements; how exact they have to be, the bound alone decides.
No kernel may reach another device: no remote copies, remote signals or barrier semaphores. Data moves between devices by JAX's collectives and lax.ppermute only.
A program may use at most 64 MiB of HBM per device.

```python
import math
import jax
import jax.numpy as jnp
from jax import lax

HARMS = 6
HARM_COLS = 13
STEPS = 1024
BAND = 720
CELLS = 23040
N_SPAN = 32


def calendar_days(key):
    return jax.random.randint(jax.random.fold_in(key, 11), (STEPS,), 0, 365).astype(jnp.int32)


def draw_day_table(key, part):
    return calendar_days(key)


def draw_band_owner(key, part):
    quads = N_SPAN // 4
    half = N_SPAN // 2
    kinds = jax.random.randint(jax.random.fold_in(key, 51), (quads,), 0, 4).astype(jnp.int32)
    first = jax.random.randint(jax.random.fold_in(key, 52), (), 0, quads).astype(jnp.int32)
    second = ((first + 1 + jax.random.randint(jax.random.fold_in(key, 53), (), 0, quads - 1)) % quads).astype(jnp.int32)
    kinds = kinds.at[first].set(0).at[second].set(1)
    index = jnp.arange(quads, dtype=jnp.int32)
    first_a = 2 * index
    first_b = 2 * index + 1
    first_c = 2 * index + half
    first_d = 2 * index + 1 + half
    owner_a = jnp.select([kinds == 0, kinds == 1, kinds == 2], [first_b, first_c, first_b], first_c)
    owner_b = jnp.select([kinds == 0, kinds == 1, kinds == 2], [first_d, first_a, first_a], first_d)
    owner_c = jnp.select([kinds == 0, kinds == 1, kinds == 2], [first_a, first_d, first_d], first_a)
    owner_d = jnp.select([kinds == 0, kinds == 1, kinds == 2], [first_c, first_b, first_c], first_b)
    owner = jnp.zeros((N_SPAN,), jnp.int32)
    owner = owner.at[first_a].set(owner_a).at[first_b].set(owner_b)
    owner = owner.at[first_c].set(owner_c).at[first_d].set(owner_d)
    return owner.astype(jnp.int32)


def draw_field(key, part):
    day_values = calendar_days(key)
    angles = day_values.astype(jnp.float32) * (2.0 * math.pi / 365.0)
    basis_rows = [jnp.ones_like(angles)]
    for order in range(1, HARMS + 1):
        basis_rows.append(jnp.cos(order * angles))
        basis_rows.append(jnp.sin(order * angles))
    design = jnp.stack(basis_rows, 0)
    amplitude = jax.random.normal(jax.random.fold_in(key, 21), (HARM_COLS, CELLS), jnp.float32)
    noise_scale = jnp.exp(jax.random.uniform(jax.random.fold_in(key, 31), (CELLS,), jnp.float32, math.log(0.3), math.log(3.0)))
    noise_part = jax.random.normal(jax.random.fold_in(key, 41), (STEPS, CELLS), jnp.float32)
    signal = jnp.dot(design.T, amplitude, precision=lax.Precision.HIGHEST)
    return jnp.clip(signal + noise_part * noise_scale[None, :], -60.0, 60.0)


def plant(entries, own_key, low, largest):
    index_at = [jax.random.randint(jax.random.fold_in(own_key, axis), (), 0, length) for axis, length in enumerate(entries.shape)]
    widest = entries.shape.index(max(entries.shape))
    next_to = index_at[:widest] + [(index_at[widest] + 1) % entries.shape[widest]] + index_at[widest + 1:]
    return entries.at[tuple(index_at)].set(low).at[tuple(next_to)].set(largest)


def setup_inputs(seed: int = 0, part: int = 0) -> dict:
    streams_of = jax.random.split(jax.random.key(seed), 5)
    own_keys = jax.random.split(jax.random.fold_in(streams_of[4], part), 5)
    return {
        "field": draw_field(jax.random.fold_in(jax.random.fold_in(streams_of[4], part), 71), part),
        "day_table": draw_day_table(jax.random.fold_in(jax.random.fold_in(streams_of[4], part), 71), part),
        "band_owner": draw_band_owner(jax.random.fold_in(jax.random.fold_in(streams_of[4], part), 71), part),
        "sea_mask": plant((jax.random.randint(streams_of[3], (CELLS,), 0, 3) < 2).astype(jnp.int32), jax.random.fold_in(streams_of[3], 1), 0, 1),
    }


def harmonic_basis(day_values):
    angles = day_values.astype(jnp.float32) * (2.0 * math.pi / 365.0)
    basis_rows = [jnp.ones_like(angles)]
    for order in range(1, HARMS + 1):
        basis_rows.append(jnp.cos(order * angles))
        basis_rows.append(jnp.sin(order * angles))
    return jnp.stack(basis_rows, 0)

def reference(field, day_table, band_owner, sea_mask):
    design = harmonic_basis(day_table)
    gram_matrix = jnp.dot(design, design.T, precision=lax.Precision.HIGHEST)
    factor = jnp.linalg.cholesky(gram_matrix)
    projection = jnp.dot(design, field, precision=lax.Precision.HIGHEST)
    coeffs = jax.scipy.linalg.cho_solve((factor, True), projection)
    residual = field - jnp.dot(design.T, coeffs, precision=lax.Precision.HIGHEST)
    variance = jnp.sum(residual * residual, axis=0) / design.shape[1]
    weight_mask = sea_mask.astype(jnp.float32)
    coeffs = coeffs * weight_mask[None, :]
    variance = variance * weight_mask
    slots = jnp.arange(N_SPAN, dtype=jnp.int32)
    source_band = jnp.zeros((N_SPAN,), jnp.int32).at[band_owner].set(slots)
    coeff_out = coeffs.reshape(HARM_COLS, N_SPAN, BAND)[:, source_band, :].reshape(HARM_COLS, CELLS)
    variance_out = variance.reshape(N_SPAN, BAND)[source_band, :].reshape(CELLS)
    return (coeff_out, variance_out)
```

```python
import functools
import math

import jax
import jax.numpy as jnp
from jax import lax
from jax.experimental import pallas as pl
from jax.experimental.pallas import tpu as pltpu
from jax.sharding import PartitionSpec as P

HARMS = 6
LANES = 128
ROWS = 16


def harmonic_basis(day_values):
    angles = day_values.astype(jnp.float32) * (2.0 * math.pi / 365.0)
    basis_rows = [jnp.ones_like(angles)]
    for order in range(1, HARMS + 1):
        basis_rows.append(jnp.cos(order * angles))
        basis_rows.append(jnp.sin(order * angles))
    return jnp.stack(basis_rows, 0)


def split_radices(groups):
    radices = []
    rest = groups
    if rest % 2 == 0:
        radices.append(2)
        rest //= 2
    while rest % 4 == 0:
        radices.append(4)
        rest //= 4
    if rest > 1 or not radices:
        radices.append(rest)
    return radices


def round_up(value, unit):
    return -(-value // unit) * unit


def chunk_of(cells, most):
    tiles = cells // LANES
    best = max(t for t in range(1, tiles + 1) if tiles % t == 0 and t * LANES <= most)
    return best * LANES


def rounded(x):
    return lax.reduce_precision(x, 8, 7)


def split_design(design, steps_dev):
    d = jnp.pad(design, ((0, ROWS - design.shape[0]), (0, 0)))
    high = rounded(d)
    mid = rounded(d - high)
    low = rounded(d - high - mid)
    none = jnp.zeros_like(d)
    stacked = jnp.concatenate(
        [
            jnp.concatenate([high, high, high], 1),
            jnp.concatenate([mid, mid, none], 1),
            jnp.concatenate([low, none, none], 1),
        ],
        0,
    )
    return stacked.astype(jnp.bfloat16)


def sums_kernel(order_ref, lhs_ref, field_ref, *refs, cols, band, width, chunk, lead):
    outs, scratch = refs[:-1], refs[-1]
    step = pl.program_id(0)
    f = field_ref[...]
    high = f.astype(jnp.bfloat16)
    left = f - high.astype(jnp.float32)
    mid = left.astype(jnp.bfloat16)
    low = (left - mid.astype(jnp.float32)).astype(jnp.bfloat16)
    stacked = jnp.concatenate([high, mid, low], 0)
    parts = jnp.dot(lhs_ref[...], stacked, preferred_element_type=jnp.float32)
    total = parts[:ROWS] + (parts[ROWS : 2 * ROWS] + parts[2 * ROWS :])
    squares = jnp.sum(f * f, axis=0, keepdims=True)
    row = lax.broadcasted_iota(jnp.int32, total.shape, 0)
    scratch[:, pl.ds(pl.multiple_of(step * chunk, LANES), chunk)] = jnp.where(
        row == cols, squares, total
    )

    @pl.when(step == pl.num_programs(0) - 1)
    def _():
        edge = scratch.shape[1] - 2 * LANES
        scratch[:, edge:] = jnp.zeros((ROWS, 2 * LANES), jnp.float32)
        for q in range(lead * len(outs)):
            start = order_ref[q] * band
            offset = lax.rem(start, LANES)
            base = pl.multiple_of(start - offset, LANES)
            window = scratch[:, pl.ds(base, width + LANES)]
            span = width + LANES
            rolled = pltpu.roll(window, lax.rem(span - offset, span), 1)
            outs[q // lead][q % lead] = rolled[:, :width]


def fit_kernel(inv_ref, invt_ref, mask_ref, *refs, cols, band, steps):
    parts, coeff_ref, var_ref = refs[:-2], refs[-2], refs[-1]
    total = parts[0][0]
    for part in parts[1:]:
        total = total + part[0]
    hp = lax.Precision.HIGHEST
    half = jnp.dot(inv_ref[...], total, precision=hp, preferred_element_type=jnp.float32)
    coeffs = jnp.dot(invt_ref[...], half, precision=hp, preferred_element_type=jnp.float32)
    squares = total[cols : cols + 1]
    rest = squares - jnp.sum(half * half, axis=0, keepdims=True)
    variance = jnp.maximum(rest, 0.0) / steps
    mask = mask_ref[...]
    coeff_ref[...] = coeffs[:cols, :band] * mask
    var_ref[...] = variance[:, :band] * mask


def on_device(field, day_table, band_owner, sea_mask):
    groups = lax.axis_size("span")
    own_index = lax.axis_index("span")
    steps_dev, cells = field.shape
    band = cells // groups
    width = round_up(band, LANES)
    steps = day_table.shape[0]
    radices = split_radices(groups)
    strides = [math.prod(radices[:r]) for r in range(len(radices))]

    slots = jnp.arange(groups, dtype=jnp.int32)
    target = jnp.zeros_like(slots)
    inner = groups
    for radix, stride in zip(radices, strides):
        inner //= radix
        target = target + ((slots // inner + own_index // stride) % radix) * stride
    order = jnp.sum(
        jnp.where(band_owner[None, :] == target[:, None], slots[None, :], 0), axis=1
    )
    days = lax.dynamic_slice_in_dim(day_table, own_index * steps_dev, steps_dev)
    own_design = harmonic_basis(days)
    cols = own_design.shape[0]
    lhs = split_design(own_design, steps_dev)

    lead = groups // radices[0]
    chunk = chunk_of(cells, 4608)
    pieces = pl.pallas_call(
        functools.partial(
            sums_kernel, cols=cols, band=band, width=width, chunk=chunk, lead=lead
        ),
        grid_spec=pltpu.PrefetchScalarGridSpec(
            num_scalar_prefetch=1,
            grid=(cells // chunk,),
            in_specs=[
                pl.BlockSpec(lhs.shape, lambda s, o: (0, 0)),
                pl.BlockSpec((steps_dev, chunk), lambda s, o: (0, s)),
            ],
            out_specs=[pl.BlockSpec((lead, ROWS, width), lambda s, o: (0, 0, 0))] * radices[0],
            scratch_shapes=[pltpu.VMEM((ROWS, cells + 2 * LANES), jnp.float32)],
        ),
        out_shape=[jax.ShapeDtypeStruct((lead, ROWS, width), jnp.float32)] * radices[0],
        name="sums",
    )(order, lhs, field)

    design = harmonic_basis(day_table)
    gram = jnp.dot(design, design.T, precision=lax.Precision.HIGHEST)
    factor = jnp.linalg.cholesky(gram)
    inverse = lax.linalg.triangular_solve(
        factor, jnp.eye(cols, dtype=jnp.float32), left_side=True, lower=True
    )
    inverse = jnp.pad(inverse, ((0, ROWS - cols), (0, ROWS - cols)))
    own_band = jnp.sum(jnp.where(band_owner == own_index, slots, 0))
    mask = lax.dynamic_slice_in_dim(sea_mask, own_band * band, band).astype(jnp.float32)

    pieces = list(pieces)
    for r, (radix, stride) in enumerate(zip(radices, strides)):
        received = []
        for shift in range(1, radix):
            pairs = []
            for source in range(groups):
                digit = source // stride % radix
                pairs.append((source, source + ((digit + shift) % radix - digit) * stride))
            received.append(lax.ppermute(pieces[shift], "span", pairs))
        pieces = [pieces[0]] + received
        if r + 1 < len(radices):
            total = functools.reduce(jnp.add, pieces)
            part = total.shape[0] // radices[r + 1]
            pieces = [total[k * part : (k + 1) * part] for k in range(radices[r + 1])]

    coeffs, variance = pl.pallas_call(
        functools.partial(fit_kernel, cols=cols, band=band, steps=steps),
        out_shape=[
            jax.ShapeDtypeStruct((cols, band), jnp.float32),
            jax.ShapeDtypeStruct((1, band), jnp.float32),
        ],
        name="fit",
    )(inverse, inverse.T, mask[None, :], *pieces)
    return (coeffs, variance.reshape(band))


def solution(mesh):
    in_specs = (P(("member", "span"), None), P("member"), P("member"), P())
    out_specs = (P(None, ("member", "span")), P(("member", "span")))
    return jax.shard_map(
        on_device, mesh=mesh, in_specs=in_specs, out_specs=out_specs, check_vma=False
    )
```

```python
import functools
import math

import jax
import jax.numpy as jnp
from jax import lax
from jax.experimental import pallas as pl
from jax.experimental.pallas import tpu as pltpu
from jax.sharding import PartitionSpec as P

HARMS = 6
LANES = 128
ROWS = 16


def harmonic_basis(day_values):
    angles = day_values.astype(jnp.float32) * (2.0 * math.pi / 365.0)
    basis_rows = [jnp.ones_like(angles)]
    for order in range(1, HARMS + 1):
        basis_rows.append(jnp.cos(order * angles))
        basis_rows.append(jnp.sin(order * angles))
    return jnp.stack(basis_rows, 0)


def split_radices(groups):
    radices = []
    rest = groups
    if rest % 2 == 0:
        radices.append(2)
        rest //= 2
    while rest % 4 == 0:
        radices.append(4)
        rest //= 4
    if rest > 1 or not radices:
        radices.append(rest)
    return radices


def round_up(value, unit):
    return -(-value // unit) * unit


def chunk_of(cells, most):
    tiles = cells // LANES
    best = max(t for t in range(1, tiles + 1) if tiles % t == 0 and t * LANES <= most)
    return best * LANES


def split_design(days, steps_dev, cols):
    lanes = days.shape[1]
    lane = lax.broadcasted_iota(jnp.int32, (ROWS, lanes), 1)
    row = lax.broadcasted_iota(jnp.int32, (ROWS, lanes), 0)
    angles = days * (2.0 * math.pi / 365.0)
    multiple = ((row + 1) // 2).astype(jnp.float32)
    argument = multiple * angles
    design = jnp.where(row % 2 == 1, jnp.cos(argument), jnp.sin(argument))
    design = jnp.where(row == 0, 1.0, design)
    design = jnp.where((row < cols) & (lane < 3 * steps_dev), design, 0.0)
    high = design.astype(jnp.bfloat16).astype(jnp.float32)
    mid = (design - high).astype(jnp.bfloat16).astype(jnp.float32)
    low = design - high - mid
    mid = jnp.where(lane < 2 * steps_dev, mid, 0.0)
    low = jnp.where(lane < steps_dev, low, 0.0)
    return jnp.concatenate([high, mid, low], 0).astype(jnp.bfloat16)


def own_days(days_ref, own_index, steps_dev):
    lanes = round_up(3 * steps_dev, LANES)
    start = own_index * steps_dev
    offset = lax.rem(start, LANES)
    window = days_ref[:, pl.ds(pl.multiple_of(start - offset, LANES), LANES)]
    window = jnp.broadcast_to(window.astype(jnp.float32), (ROWS, LANES))
    first = pltpu.roll(window, lax.rem(LANES - offset, LANES), 1)
    lane = lax.broadcasted_iota(jnp.int32, (ROWS, LANES), 1)
    second = pltpu.roll(first, steps_dev, 1)
    third = pltpu.roll(first, 2 * steps_dev, 1)
    days = jnp.where(lane < steps_dev, first, jnp.where(lane < 2 * steps_dev, second, third))
    return days[:, :lanes]


def sums_kernel(
    owner_ref, days_ref, field_ref, *refs, cols, band, width, chunk, lead, steps_dev, radices
):
    outs, lhs_ref, scratch = refs[:-2], refs[-2], refs[-1]
    step = pl.program_id(0)
    own_index = lax.axis_index("span")

    @pl.when(step == 0)
    def _():
        days = own_days(days_ref, own_index, steps_dev)
        lhs_ref[...] = split_design(days, steps_dev, cols)

    f = field_ref[...]
    high = f.astype(jnp.bfloat16)
    left = f - high.astype(jnp.float32)
    mid = left.astype(jnp.bfloat16)
    low = (left - mid.astype(jnp.float32)).astype(jnp.bfloat16)
    stacked = jnp.concatenate([high, mid, low], 0)
    parts = jnp.dot(
        lhs_ref[:, : 3 * steps_dev], stacked, preferred_element_type=jnp.float32
    )
    total = parts[:ROWS] + (parts[ROWS : 2 * ROWS] + parts[2 * ROWS :])
    squares = jnp.sum(f * f, axis=0, keepdims=True)
    row = lax.broadcasted_iota(jnp.int32, total.shape, 0)
    scratch[:, pl.ds(pl.multiple_of(step * chunk, LANES), chunk)] = jnp.where(
        row == cols, squares, total
    )

    @pl.when(step == pl.num_programs(0) - 1)
    def _():
        edge = scratch.shape[1] - 2 * LANES
        scratch[:, edge:] = jnp.zeros((ROWS, 2 * LANES), jnp.float32)
        for q in range(lead * len(outs)):
            start = q * band
            offset = start % LANES
            base = start - offset
            if offset:
                span = width + LANES
                block = pltpu.roll(scratch[:, base : base + span], span - offset, 1)[:, :width]
            else:
                block = scratch[:, base : base + width]
            target, source = owner_ref[q], own_index
            place, inner, first = 0, lead, None
            for radix in radices:
                digit = lax.rem(lax.rem(target, radix) - lax.rem(source, radix) + radix, radix)
                target, source = lax.div(target, radix), lax.div(source, radix)
                if first is None:
                    first = digit
                else:
                    inner //= radix
                    place = place + digit * inner
            for k, out in enumerate(outs):

                @pl.when(first == k)
                def _(out=out, block=block, place=place):
                    out[place] = block


def on_device(field, day_table, band_owner, sea_mask):
    groups = lax.axis_size("span")
    own_index = lax.axis_index("span")
    steps_dev, cells = field.shape
    band = cells // groups
    width = round_up(band, LANES)
    steps = day_table.shape[0]
    radices = split_radices(groups)
    strides = [math.prod(radices[:r]) for r in range(len(radices))]

    cols = 2 * HARMS + 1
    lead = groups // radices[0]
    chunk = chunk_of(cells, 4608)
    lanes = round_up(3 * steps_dev, LANES)
    pieces = pl.pallas_call(
        functools.partial(
            sums_kernel,
            cols=cols,
            band=band,
            width=width,
            chunk=chunk,
            lead=lead,
            steps_dev=steps_dev,
            radices=radices,
        ),
        grid_spec=pltpu.PrefetchScalarGridSpec(
            num_scalar_prefetch=1,
            grid=(cells // chunk,),
            in_specs=[
                pl.BlockSpec((1, steps), lambda s, o: (0, 0)),
                pl.BlockSpec((steps_dev, chunk), lambda s, o: (0, s)),
            ],
            out_specs=[pl.BlockSpec((lead, ROWS, width), lambda s, o: (0, 0, 0))] * radices[0],
            scratch_shapes=[
                pltpu.VMEM((3 * ROWS, lanes), jnp.bfloat16),
                pltpu.VMEM((ROWS, cells + 2 * LANES), jnp.float32),
            ],
        ),
        out_shape=[jax.ShapeDtypeStruct((lead, ROWS, width), jnp.float32)] * radices[0],
        name="sums",
    )(band_owner, day_table[None, :], field)

    slots = jnp.arange(groups, dtype=jnp.int32)
    pieces = list(pieces)
    for r, (radix, stride) in enumerate(zip(radices, strides)):
        received = []
        for shift in range(1, radix):
            pairs = []
            for source in range(groups):
                digit = source // stride % radix
                pairs.append((source, source + ((digit + shift) % radix - digit) * stride))
            received.append(lax.ppermute(pieces[shift], "span", pairs))
        pieces = [pieces[0]] + received
        total = functools.reduce(jnp.add, pieces)
        if r == 0:
            late_days, total = lax.optimization_barrier((day_table, total))
        if r + 1 < len(radices):
            part = total.shape[0] // radices[r + 1]
            pieces = [total[k * part : (k + 1) * part] for k in range(radices[r + 1])]

    design = harmonic_basis(late_days)
    gram = jnp.dot(design, design.T, precision=lax.Precision.HIGHEST)
    factor = jnp.linalg.cholesky(gram)
    inverse = lax.linalg.triangular_solve(
        factor, jnp.eye(cols, dtype=jnp.float32), left_side=True, lower=True
    )
    own_band = jnp.sum(jnp.where(band_owner == own_index, slots, 0))
    mask = lax.dynamic_slice_in_dim(sea_mask, own_band * band, band).astype(jnp.float32)

    total = total[0, :, :band]
    half = jnp.dot(inverse, total[:cols], precision=lax.Precision.HIGHEST)
    coeffs = jnp.dot(inverse.T, half, precision=lax.Precision.HIGHEST)
    rest = total[cols] - jnp.sum(half * half, axis=0)
    variance = jnp.maximum(rest, 0.0) / steps
    return (coeffs * mask[None, :], variance * mask)


def solution(mesh):
    in_specs = (P(("member", "span"), None), P("member"), P("member"), P())
    out_specs = (P(None, ("member", "span")), P(("member", "span")))
    return jax.shard_map(
        on_device, mesh=mesh, in_specs=in_specs, out_specs=out_specs, check_vma=False
    )
```

```python
import functools
import math

import jax
import jax.numpy as jnp
from jax import lax
from jax.experimental import pallas as pl
from jax.experimental.pallas import tpu as pltpu
from jax.sharding import PartitionSpec as P

HARMS = 6
LANES = 128
ROWS = 16


def sine_of_turns(turns):
    turns = turns - jnp.floor(turns + 0.5)
    turns = jnp.where(turns > 0.25, 0.5 - turns, jnp.where(turns < -0.25, -0.5 - turns, turns))
    x = turns * (2.0 * math.pi)
    square = x * x
    value = jnp.full_like(x, 1.0 / math.factorial(13))
    for power in (11, 9, 7, 5, 3, 1):
        value = value * square + (-1.0) ** (power // 2) / math.factorial(power)
    return value * x


def basis_rows(days, rows):
    row = lax.broadcasted_iota(jnp.int32, (rows, days.shape[-1]), 0)
    multiple = ((row + 1) // 2).astype(jnp.float32)
    whole = multiple * days
    whole = whole - 365.0 * jnp.floor(whole * (1.0 / 365.0))
    quarter = jnp.where(row % 2 == 1, 0.25, 0.0)
    values = sine_of_turns(whole * (1.0 / 365.0) + quarter)
    return jnp.where(row == 0, 1.0, values)


def split_radices(groups):
    radices = []
    rest = groups
    if rest % 2 == 0:
        radices.append(2)
        rest //= 2
    while rest % 4 == 0:
        radices.append(4)
        rest //= 4
    if rest > 1 or not radices:
        radices.append(rest)
    return radices


def round_up(value, unit):
    return -(-value // unit) * unit


def chunk_of(cells, most):
    tiles = cells // LANES
    best = max(t for t in range(1, tiles + 1) if tiles % t == 0 and t * LANES <= most)
    return best * LANES


def split_design(days, steps_dev, cols):
    lanes = days.shape[1]
    lane = lax.broadcasted_iota(jnp.int32, (ROWS, lanes), 1)
    row = lax.broadcasted_iota(jnp.int32, (ROWS, lanes), 0)
    design = basis_rows(days, ROWS)
    design = jnp.where((row < cols) & (lane < 3 * steps_dev), design, 0.0)
    high = design.astype(jnp.bfloat16).astype(jnp.float32)
    mid = (design - high).astype(jnp.bfloat16).astype(jnp.float32)
    low = design - high - mid
    mid = jnp.where(lane < 2 * steps_dev, mid, 0.0)
    low = jnp.where(lane < steps_dev, low, 0.0)
    return jnp.concatenate([high, mid, low], 0).astype(jnp.bfloat16)


def own_days(days_ref, own_index, steps_dev):
    lanes = round_up(3 * steps_dev, LANES)
    start = own_index * steps_dev
    offset = lax.rem(start, LANES)
    window = days_ref[:, pl.ds(pl.multiple_of(start - offset, LANES), LANES)]
    window = jnp.broadcast_to(window.astype(jnp.float32), (ROWS, LANES))
    first = pltpu.roll(window, lax.rem(LANES - offset, LANES), 1)
    lane = lax.broadcasted_iota(jnp.int32, (ROWS, LANES), 1)
    second = pltpu.roll(first, steps_dev, 1)
    third = pltpu.roll(first, 2 * steps_dev, 1)
    days = jnp.where(lane < steps_dev, first, jnp.where(lane < 2 * steps_dev, second, third))
    return days[:, :lanes]


def sums_kernel(
    owner_ref,
    days_ref,
    field_ref,
    out_ref,
    lhs_ref,
    staged,
    scratch,
    sems,
    *,
    cols,
    band,
    width,
    chunk,
    steps_dev,
    radices,
):
    own_index = lax.axis_index("span")
    cells = field_ref.shape[1]
    groups = out_ref.shape[0]
    copies = []
    for c in range(cells // chunk):
        part = pl.ds(c * chunk, chunk)
        copy = pltpu.make_async_copy(field_ref.at[:, part], staged.at[:, part], sems.at[c])
        copy.start()
        copies.append(copy)
    lhs_ref[...] = split_design(own_days(days_ref, own_index, steps_dev), steps_dev, cols)
    scratch[:, cells:] = jnp.zeros((ROWS, scratch.shape[1] - cells), jnp.float32)
    lhs = lhs_ref[:, : 3 * steps_dev]
    placed = 0
    for c, copy in enumerate(copies):
        copy.wait()
        f = staged[:, c * chunk : (c + 1) * chunk]
        high = f.astype(jnp.bfloat16)
        left = f - high.astype(jnp.float32)
        mid = left.astype(jnp.bfloat16)
        low = (left - mid.astype(jnp.float32)).astype(jnp.bfloat16)
        stacked = jnp.concatenate([high, mid, low], 0)
        parts = jnp.dot(lhs, stacked, preferred_element_type=jnp.float32)
        total = parts[:ROWS] + (parts[ROWS : 2 * ROWS] + parts[2 * ROWS :])
        squares = jnp.sum(f * f, axis=0, keepdims=True)
        row = lax.broadcasted_iota(jnp.int32, total.shape, 0)
        scratch[:, c * chunk : (c + 1) * chunk] = jnp.where(row == cols, squares, total)
        while placed < groups and (placed + 1) * band <= (c + 1) * chunk:
            start = placed * band
            offset = start % LANES
            base = start - offset
            if offset:
                span = width + LANES
                block = pltpu.roll(scratch[:, base : base + span], span - offset, 1)[:, :width]
            else:
                block = scratch[:, base : base + width]
            target, source = owner_ref[placed], own_index
            place, inner = 0, groups
            for radix in radices:
                digit = lax.rem(lax.rem(target, radix) - lax.rem(source, radix) + radix, radix)
                target, source = lax.div(target, radix), lax.div(source, radix)
                inner //= radix
                place = place + digit * inner
            out_ref[place] = block
            placed += 1


def on_device(field, day_table, band_owner, sea_mask):
    groups = lax.axis_size("span")
    own_index = lax.axis_index("span")
    steps_dev, cells = field.shape
    band = cells // groups
    width = round_up(band, LANES)
    steps = day_table.shape[0]
    radices = split_radices(groups)
    strides = [math.prod(radices[:r]) for r in range(len(radices))]

    cols = 2 * HARMS + 1
    chunk = chunk_of(cells, 4608)
    lanes = round_up(3 * steps_dev, LANES)
    sums = pl.pallas_call(
        functools.partial(
            sums_kernel,
            cols=cols,
            band=band,
            width=width,
            chunk=chunk,
            steps_dev=steps_dev,
            radices=radices,
        ),
        in_specs=[
            pl.BlockSpec(memory_space=pltpu.SMEM),
            pl.BlockSpec(memory_space=pltpu.VMEM),
            pl.BlockSpec(memory_space=pl.ANY),
        ],
        out_specs=pl.BlockSpec(memory_space=pltpu.VMEM),
        out_shape=pltpu.VMEM((groups, ROWS, width), jnp.float32),
        scratch_shapes=[
            pltpu.VMEM((3 * ROWS, lanes), jnp.bfloat16),
            pltpu.VMEM((steps_dev, cells), jnp.float32),
            pltpu.VMEM((ROWS, cells + 2 * LANES), jnp.float32),
            pltpu.SemaphoreType.DMA((cells // chunk,)),
        ],
        name="sums",
    )(band_owner, day_table[None, :], field)

    slots = jnp.arange(groups, dtype=jnp.int32)
    lead = groups // radices[0]
    pieces = [sums[k * lead : (k + 1) * lead] for k in range(radices[0])]
    for r, (radix, stride) in enumerate(zip(radices, strides)):
        received = []
        for shift in range(1, radix):
            pairs = []
            for source in range(groups):
                digit = source // stride % radix
                pairs.append((source, source + ((digit + shift) % radix - digit) * stride))
            received.append(lax.ppermute(pieces[shift], "span", pairs))
        pieces = [pieces[0]] + received
        total = functools.reduce(jnp.add, pieces)
        if r == 0:
            late_days, total = lax.optimization_barrier((day_table, total))
        if r + 1 < len(radices):
            part = total.shape[0] // radices[r + 1]
            pieces = [total[k * part : (k + 1) * part] for k in range(radices[r + 1])]

    design = basis_rows(late_days[None, :].astype(jnp.float32), cols)
    gram = jnp.dot(design, design.T, precision=lax.Precision.HIGHEST)
    factor = jnp.linalg.cholesky(gram)
    inverse = lax.linalg.triangular_solve(
        factor, jnp.eye(cols, dtype=jnp.float32), left_side=True, lower=True
    )
    own_band = jnp.sum(jnp.where(band_owner == own_index, slots, 0))
    mask = lax.dynamic_slice_in_dim(sea_mask, own_band * band, band).astype(jnp.float32)
    mask = lax.optimization_barrier(mask)

    total = total[0, :, :band]
    half = jnp.dot(inverse, total[:cols], precision=lax.Precision.HIGHEST)
    coeffs = jnp.dot(inverse.T, half, precision=lax.Precision.HIGHEST)
    rest = total[cols] - jnp.sum(half * half, axis=0)
    variance = jnp.maximum(rest, 0.0) / steps
    return (coeffs * mask[None, :], variance * mask)


def solution(mesh):
    in_specs = (P(("member", "span"), None), P("member"), P("member"), P())
    out_specs = (P(None, ("member", "span")), P(("member", "span")))
    return jax.shard_map(
        on_device, mesh=mesh, in_specs=in_specs, out_specs=out_specs, check_vma=False
    )
```
